256 devices in a mesh: grp: 32 (over x, z), sub: 8 (over y, core).
Axes of the slice: x: 4, y: 4, z: 8, core: 2. Of those that a mesh axis runs over, the one named last changes fastest.
Arguments:
- ham_columns: bfloat16 [768, 5, 128, 128], P(('grp', 'sub')), may hold values from -2.2 to 2.2, as said below
- bond_mask: int32 [768, 4], P(('grp', 'sub')), may hold values 0 or 1
- owned_counts: int32 [32, 8], replicated, may hold values from 1 to 3, as said below
- fermi_level: float32 [1], replicated, may hold values from -0.5 to 0.5
Outputs:
- density: bfloat16 [768, 9, 128, 128], P(('grp', 'sub'))
The draws below stay inside these ranges and needn't reach their ends.
Inputs may be any that keep to these rules, and one draw needn't show every extreme that they name: `ham_columns`: block 0 of every stored block column is symmetric. `bond_mask`: bond lists of slots that hold no cluster are never read. `owned_counts`: along sub, the devices 2k and 2k + 1 of a group own 2 * 2 block columns together, so group g owns clusters g * 16 to (g + 1) * 16 - 1, handed to its devices in order along sub in consecutive runs; no device owns exactly 2; every row has a device that owns 3.
All inputs are finite; a program needn't handle non-finite values. No bound on the sum of `bond_mask` on one device may be relied on, other than what follows from the above.
Results may differ from the reference program's by a relative error of at most 0.0025.
Values may be sent and summed in bfloat16 or wider, within the bound.
No kernel may reach another device: no remote copies, remote signals or barrier semaphores. Data moves between devices by JAX's collectives and lax.ppermute only.
A program may use at most 64 MiB of HBM per device.

```python
import jax
import jax.numpy as jnp
from jax import lax

BS = 128
COLS_MEAN = 2
REACH = 4
CMAX = 3
NBC = 512
SLOTS = 768
N_GRP = 32
N_SUB = 8


def draw_ham_columns(key, part):
    base_key = jax.random.fold_in(key, 11)
    couple_key, energy_key = jax.random.split(base_key, 2)
    shape_all = (SLOTS, REACH + 1, BS, BS)
    couplings = jax.random.truncated_normal(couple_key, -4.0, 4.0, shape_all, jnp.float32) * 0.03
    energies = jax.random.uniform(energy_key, (SLOTS, BS), jnp.float32, -2.0, 2.0)
    diagonal = couplings[:, 0]
    symmetric = (diagonal + jnp.swapaxes(diagonal, 1, 2)) * 0.70710677
    eye_mask = jnp.eye(BS, dtype=jnp.float32)
    center_block = symmetric + eye_mask[None, :, :] * energies[:, :, None]
    columns = jnp.concatenate([center_block[:, None], couplings[:, 1:]], axis=1)
    return columns.astype(jnp.bfloat16)


def draw_owned_counts(key, part):
    base_key = jax.random.fold_in(key, 23)
    sign_key, extra_key, forced_key = jax.random.split(base_key, 3)
    pair_count = N_SUB // 2
    sign_values = jax.random.randint(sign_key, (N_GRP, pair_count), 0, 2).astype(jnp.int32) * 2 - 1
    extra = jax.random.randint(extra_key, (N_GRP, pair_count), 0, COLS_MEAN - 1).astype(jnp.int32) + 1
    forced = jax.random.randint(forced_key, (N_GRP,), 0, pair_count).astype(jnp.int32)
    is_forced = jnp.arange(pair_count, dtype=jnp.int32)[None, :] == forced[:, None]
    extra = jnp.where(is_forced, COLS_MEAN - 1, extra)
    sign_values = jnp.where(is_forced, 1, sign_values)
    first_count = COLS_MEAN + sign_values * extra
    second_count = 2 * COLS_MEAN - first_count
    paired = jnp.stack([first_count, second_count], axis=2)
    return paired.reshape(N_GRP, N_SUB).astype(jnp.int32)


def touch_ends(drawn, own_key, least, top_value):
    extent = drawn.shape
    place = [jax.random.randint(jax.random.fold_in(own_key, axis), (), 0, extent[axis]) for axis in range(len(extent))]
    drawn = drawn.at[tuple(place)].set(least)
    longest = extent.index(max(extent))
    place[longest] = (place[longest] + 1) % extent[longest]
    return drawn.at[tuple(place)].set(top_value)


def setup_inputs(seed: int = 0) -> dict:
    splits = jax.random.split(jax.random.key(seed), 5)
    ham_columns = draw_ham_columns(jax.random.fold_in(splits[4], 71), 0)
    bond_mask = touch_ends((jax.random.randint(splits[1], (SLOTS, REACH), 0, 2) < 1).astype(jnp.int32), jax.random.fold_in(splits[1], 1), 0, 1)
    owned_counts = draw_owned_counts(jax.random.fold_in(splits[4], 71), 0)
    fermi_level = jnp.clip(jax.random.uniform(splits[3], (1,), jnp.float32, -0.5, 0.5), -0.5, 0.5)
    return {"ham_columns": ham_columns, "bond_mask": bond_mask, "owned_counts": owned_counts, "fermi_level": fermi_level}


spectral_span = 4.0


def build_tile(window_cols, window_bonds, chemical):
    reach_len = window_bonds.shape[1]
    window_len = window_cols.shape[0]
    block_width = window_cols.shape[2]
    center = reach_len
    identity = jnp.eye(block_width, dtype=jnp.float32)
    bond_values = window_bonds.astype(jnp.float32)
    living = []
    for member in range(window_len):
        if member == center:
            living.append(jnp.ones((), jnp.float32))
        elif member > center:
            living.append(bond_values[center, member - center - 1])
        else:
            living.append(bond_values[member, center - member - 1])
    rows_list = []
    for row_blk in range(window_len):
        pieces = []
        for col_blk in range(window_len):
            distance = row_blk - col_blk
            weight = living[row_blk] * living[col_blk]
            if distance == 0:
                block_value = (window_cols[row_blk, 0].astype(jnp.float32) - chemical * identity) * weight
            elif 0 < distance <= reach_len:
                block_value = window_cols[col_blk, distance].astype(jnp.float32) * (weight * bond_values[col_blk, distance - 1])
            elif 0 < -distance <= reach_len:
                block_value = window_cols[row_blk, -distance].astype(jnp.float32).T * (weight * bond_values[row_blk, -distance - 1])
            else:
                block_value = jnp.zeros((block_width, block_width), jnp.float32)
            pieces.append(block_value)
        rows_list.append(jnp.concatenate(pieces, axis=1))
    return (jnp.concatenate(rows_list, axis=0) / spectral_span).astype(jnp.bfloat16)


def product(matrix, vector):
    return jnp.dot(matrix, vector.astype(jnp.bfloat16), preferred_element_type=jnp.float32)


def apply_first(matrix, vector):
    first_term = product(matrix, vector)
    second = product(matrix, first_term)
    third_term = product(matrix, second)
    return 1.5 * first_term - 0.5 * third_term


def make_selector(window_len, block_width):
    center = (window_len - 1) // 2
    above = jnp.zeros((center * block_width, block_width), jnp.float32)
    return jnp.concatenate([above, jnp.eye(block_width, dtype=jnp.float32), above], axis=0)


def density_column(matrix, selector):
    step_one = apply_first(matrix, selector)
    step_two = apply_first(matrix, step_one)
    step_three = apply_first(matrix, step_two)
    sign_column = 1.5 * step_one - 0.5 * step_three
    return (0.5 * (selector - sign_column)).astype(jnp.bfloat16)


def reference(ham_columns, bond_mask, owned_counts, fermi_level):
    block_width = ham_columns.shape[2]
    reach_len = bond_mask.shape[1]
    window_len = 2 * reach_len + 1
    slot_total = ham_columns.shape[0]
    counts_flat = owned_counts.reshape(-1).astype(jnp.int32)
    run_ends = jnp.cumsum(counts_flat).astype(jnp.int32)
    starts = run_ends - counts_flat
    positions = jnp.arange(NBC, dtype=jnp.int32)
    owner_index = jnp.sum((run_ends[None, :] <= positions[:, None]).astype(jnp.int32), axis=1).astype(jnp.int32)
    slot_of = (owner_index * CMAX + positions - starts[owner_index]).astype(jnp.int32)
    cycle_cols = jnp.take(ham_columns, slot_of, axis=0)
    cycle_bonds = jnp.take(bond_mask, slot_of, axis=0)
    selector = make_selector(window_len, block_width)
    chemical = fermi_level[0]

    def one_center(center_pos):
        window_pos = ((center_pos - reach_len + jnp.arange(window_len, dtype=jnp.int32)) % NBC).astype(jnp.int32)
        matrix = build_tile(jnp.take(cycle_cols, window_pos, axis=0), jnp.take(cycle_bonds, window_pos, axis=0), chemical)
        return density_column(matrix, selector).reshape(window_len, block_width, block_width)

    results = lax.map(one_center, positions)
    slot_ids = jnp.arange(slot_total, dtype=jnp.int32)
    device_of = (slot_ids // CMAX).astype(jnp.int32)
    within = (slot_ids % CMAX).astype(jnp.int32)
    in_use = within < counts_flat[device_of]
    center_of = jnp.minimum(starts[device_of] + within, NBC - 1).astype(jnp.int32)
    picked = jnp.take(results, center_of, axis=0)
    return jnp.where(in_use[:, None, None, None], picked, jnp.zeros_like(picked))
```

```python
import jax
import jax.numpy as jnp
from jax import lax
from jax.experimental import pallas as pl
from jax.experimental.pallas import tpu as pltpu
from jax.sharding import PartitionSpec as P

AXES = ("grp", "sub")
CHIP_COLS = 4
BF16 = jnp.bfloat16
F32 = jnp.float32


def place(counts_ref):
    group = lax.axis_index("grp")
    member = lax.axis_index("sub")
    parity = member % 2
    low_count = counts_ref[group, member - parity]
    first = jnp.where(parity == 0, 0, low_count)
    return parity, low_count, first, counts_ref[group, member]


def pack_kernel(counts_ref, bond_ref, mate_bond_ref, ham_ref, mate_ref, up_ref, down_ref):
    parity, low_count, _, _ = place(counts_ref)

    def source(t):
        in_low = t < low_count
        slot = jnp.where(in_low, t, t - low_count)
        return in_low == (parity == 0), slot

    def block(t, o, target, row):
        mine, slot = source(t)

        def put(cols, bonds):
            value = cols[slot, o]
            if o:
                value = value * (bonds[slot, o - 1] != 0).astype(F32).astype(BF16)
            target[row : row + 128, :] = value

        pl.when(mine)(lambda: put(ham_ref, bond_ref))
        pl.when(jnp.logical_not(mine))(lambda: put(mate_ref, mate_bond_ref))

    for h in range(2):
        for o in range(5):
            block(parity * 2 + h, o, up_ref, (h * 5 + o) * 128)
    rows = []
    for t in range(CHIP_COLS):
        mine, slot = source(t)
        for o in range(4):
            bit = jnp.where(mine, bond_ref[slot, o], mate_bond_ref[slot, o])
            rows.append(jnp.full((1, 128), bit.astype(F32)))
    up_ref[1280:1296, :] = jnp.concatenate(rows, axis=0).astype(BF16)

    @pl.when(parity == 0)
    def _():
        for k, (t, o) in enumerate([(0, 0), (0, 1), (0, 2), (0, 3), (3, 0)]):
            block(t, o, down_ref, k * 128)

    @pl.when(parity == 1)
    def _():
        for k, (t, o) in enumerate([(1, 0), (1, 1), (1, 2), (2, 0), (2, 1)]):
            block(t, o, down_ref, k * 128)


def main_kernel(
    counts_ref, bond_ref, mate_bond_ref, mu_ref, ham_hbm, mate_hbm, up_hbm, mate_up_hbm, down_hbm, mate_down_hbm,
    out_hbm, cols, bits_in, bits, x, first, kept, va, vb, mask, out, sems, out_sems,
):
    parity, low_count, base, count = place(counts_ref)

    copies = []
    for t in range(CHIP_COLS):
        in_low = t < low_count
        slot = jnp.where(in_low, t, t - low_count)
        mine = in_low == (parity == 0)
        own = pltpu.make_async_copy(ham_hbm.at[slot], cols.at[4 + t], sems.at[t])
        mate = pltpu.make_async_copy(mate_hbm.at[slot], cols.at[4 + t], sems.at[t])
        pl.when(mine)(own.start)
        pl.when(jnp.logical_not(mine))(mate.start)
        copies.append(own)
    for k, (ref, half) in enumerate([(up_hbm, parity), (mate_up_hbm, 1 - parity)]):
        for h in range(2):
            for o in range(5):
                c = pltpu.make_async_copy(
                    ref.at[pl.ds((h * 5 + o) * 128, 128)], cols.at[half * 2 + h, o], sems.at[5 + k * 10 + h * 5 + o]
                )
                c.start()
                copies.append(c)
    c = pltpu.make_async_copy(up_hbm.at[pl.ds(1280, 16)], bits_in, sems.at[4])
    c.start()
    copies.append(c)
    low_list = [(8, 0), (8, 1), (8, 2), (8, 3), (11, 0)]
    high_list = [(9, 0), (9, 1), (9, 2), (10, 0), (10, 1)]
    for k in range(5):
        for n, ref in enumerate([down_hbm, mate_down_hbm]):
            is_low = parity == n
            p = jnp.where(is_low, low_list[k][0], high_list[k][0])
            o = jnp.where(is_low, low_list[k][1], high_list[k][1])
            c = pltpu.make_async_copy(ref.at[pl.ds(k * 128, 128)], cols.at[p, o], sems.at[25 + k * 2 + n])
            c.start()
            copies.append(c)

    zero = jnp.zeros((128, 128), BF16)
    for i in range(12):
        for j in range(12):
            if abs(i - j) > 4 or i == 11 or j == 11:
                x[i * 128 : (i + 1) * 128, j * 128 : (j + 1) * 128] = zero
    bits[32:64, :] = jnp.zeros((32, 128), F32)
    for t in range(CHIP_COLS):
        in_low = t < low_count
        slot = jnp.where(in_low, t, t - low_count)
        mine = in_low == (parity == 0)
        for o in range(4):
            bit = jnp.where(mine, bond_ref[slot, o], mate_bond_ref[slot, o]).astype(F32)
            bits[16 + t * 4 + o : 17 + t * 4 + o, :] = jnp.full((1, 128), bit)
    for c in copies:
        c.wait()
    bits[0:16, :] = bits_in[...].astype(F32)

    one = jnp.ones((1, 128), F32)
    for i in range(3):
        c = 4 + i
        for u in range(12):
            if u == c:
                row = one
            elif c < u <= c + 4:
                row = bits[pl.ds((c + base) * 4 + (u - c - 1), 1), :]
            elif c - 4 <= u < c:
                row = bits[pl.ds((u + base) * 4 + (c - u - 1), 1), :]
            else:
                row = jnp.zeros((1, 128), F32)
            mask[i : i + 1, u * 128 : (u + 1) * 128] = row

    mu = mu_ref[0]
    eye = (
        lax.broadcasted_iota(jnp.int32, (128, 128), 0) == lax.broadcasted_iota(jnp.int32, (128, 128), 1)
    ).astype(F32)
    for u in range(11):
        p = u + base
        pc = jnp.minimum(p, 11)
        d = (cols[pc, 0].astype(F32) - mu * eye) * 0.25
        d = jnp.where(p <= 11, d, 0.0)
        x[u * 128 : (u + 1) * 128, u * 128 : (u + 1) * 128] = d.astype(BF16)
        for o in range(1, 5):
            v = u + o
            if v > 10:
                continue
            row = jnp.where(jnp.logical_and(p >= 4, p < 8), bits[pl.ds(p * 4 + o - 1, 1), :], one * 1.0)
            blk = jnp.where(p + o <= 11, cols[pc, o].astype(F32) * (row * 0.25), 0.0)
            x[v * 128 : (v + 1) * 128, u * 128 : (u + 1) * 128] = blk.astype(BF16)
            x[u * 128 : (u + 1) * 128, v * 128 : (v + 1) * 128] = blk.T.astype(BF16)

    def product(src, n, r0, r1, off=0):
        k0, k1 = max(0, n - 2), min(6, n + 3)
        acc = jnp.dot(
            src[off + r0 : off + r1, k0 * 256 : k1 * 256],
            x[k0 * 256 : k1 * 256, n * 256 : (n + 1) * 256],
            preferred_element_type=F32,
        )
        parts = []
        for i in range(r0 // 128, r1 // 128):
            m = mask[i : i + 1, n * 256 : (n + 1) * 256]
            parts.append(acc[i * 128 - r0 : (i + 1) * 128 - r0, :] * m)
        return parts

    span = [(0, 256), (0, 384), (0, 384), (0, 384), (0, 384), (256, 384)]

    def zero_rest(ref):
        ref[256:384, 0:256] = jnp.zeros((128, 256), ref.dtype)
        ref[0:256, 1280:1536] = jnp.zeros((256, 256), ref.dtype)

    zero_rest(va)
    zero_rest(vb)

    def sweep(src, off, use):
        for n in range(6):
            r0, r1 = span[n]
            parts = product(src, n, r0, r1, off)
            for i, part in zip(range(r0 // 128, r1 // 128), parts):
                use(i, n, part)

    def sl(i, n):
        return (slice(i * 128, (i + 1) * 128), slice(n * 256, (n + 1) * 256))

    def store(ref):
        def use(i, n, part):
            ref[sl(i, n)] = part.astype(BF16)

        return use

    sweep(x, 512, store(va))

    def end_one(i, n, part):
        rows = slice(512 + i * 128, 512 + (i + 1) * 128)
        s = 1.5 * x[rows, n * 256 : (n + 1) * 256].astype(F32) - 0.5 * part
        kept[sl(i, n)] = s
        vb[sl(i, n)] = s.astype(BF16)

    sweep(va, 0, end_one)

    def keep_first(ref):
        def use(i, n, part):
            first[sl(i, n)] = part
            ref[sl(i, n)] = part.astype(BF16)

        return use

    sweep(vb, 0, keep_first(va))
    sweep(va, 0, store(vb))

    def end_two(i, n, part):
        va[sl(i, n)] = (1.5 * first[sl(i, n)] - 0.5 * part).astype(BF16)

    sweep(vb, 0, end_two)
    sweep(va, 0, keep_first(vb))
    sweep(vb, 0, store(va))

    def end_three(i, n, part):
        s3 = 1.5 * first[sl(i, n)] - 0.5 * part
        y = 1.5 * kept[sl(i, n)] - 0.5 * s3
        for h in range(2):
            w = 2 * n + h - i
            if 0 <= w < 9:
                d = -0.5 * y[:, h * 128 : (h + 1) * 128]
                if w == 4:
                    d = d + 0.5 * eye
                d = jnp.where(i < count, d, 0.0)
                out[i, w] = d.T.astype(BF16)

    sweep(va, 0, end_three)
    c = pltpu.make_async_copy(out, out_hbm, out_sems.at[0])
    c.start()
    c.wait()


def shift(value, step):
    size = lax.axis_size("grp") * lax.axis_size("sub")
    return lax.ppermute(value, AXES, [(s, (s + step) % size) for s in range(size)])


def mate_of(value):
    return lax.ppermute(value, "sub", [(s, s ^ 1) for s in range(lax.axis_size("sub"))])


def body(ham_columns, bond_mask, owned_counts, fermi_level):
    smem = pl.BlockSpec(memory_space=pltpu.SMEM)
    vmem = pl.BlockSpec(memory_space=pltpu.VMEM)
    hbm = pl.BlockSpec(memory_space=pltpu.HBM)
    mate_bond = mate_of(bond_mask)
    mate_ham = mate_of(ham_columns)
    up, down = pl.pallas_call(
        pack_kernel,
        out_shape=(jax.ShapeDtypeStruct((1296, 128), BF16), jax.ShapeDtypeStruct((640, 128), BF16)),
        in_specs=[smem, smem, smem, vmem, vmem],
        out_specs=(vmem, vmem),
        name="pack",
    )(owned_counts, bond_mask, mate_bond, ham_columns, mate_ham)
    up_got = shift(up, 2)
    down_got = shift(down, -2)
    mate_down = mate_of(down_got)
    mate_up = mate_of(up_got)
    return pl.pallas_call(
        main_kernel,
        out_shape=jax.ShapeDtypeStruct((3, 9, 128, 128), BF16),
        in_specs=[smem, smem, smem, smem] + [hbm] * 6,
        out_specs=hbm,
        scratch_shapes=[
            pltpu.VMEM((12, 5, 128, 128), BF16),
            pltpu.VMEM((16, 128), BF16),
            pltpu.VMEM((64, 128), F32),
            pltpu.VMEM((1536, 1536), BF16),
            pltpu.VMEM((384, 1536), F32),
            pltpu.VMEM((384, 1536), F32),
            pltpu.VMEM((384, 1536), BF16),
            pltpu.VMEM((384, 1536), BF16),
            pltpu.VMEM((8, 1536), F32),
            pltpu.VMEM((3, 9, 128, 128), BF16),
            pltpu.SemaphoreType.DMA((35,)),
            pltpu.SemaphoreType.DMA((1,)),
        ],
        name="columns",
    )(owned_counts, bond_mask, mate_bond, fermi_level, ham_columns, mate_ham, up_got, mate_up, down_got, mate_down)


def solution(mesh):
    placed = (P(AXES, None, None, None), P(AXES, None), P(), P())
    return jax.shard_map(
        body,
        mesh=mesh,
        in_specs=placed,
        out_specs=P(AXES, None, None, None),
        check_vma=False,
    )
```

```python
import jax
import jax.numpy as jnp
from jax import lax
from jax.experimental import pallas as pl
from jax.experimental.pallas import tpu as pltpu
from jax.sharding import PartitionSpec as P

AXES = ("grp", "sub")
CHIP_COLS = 4
BF16 = jnp.bfloat16
F32 = jnp.float32

DOWN = (((0, 0), (0, 1), (0, 2), (0, 3), (3, 0)), ((1, 0), (1, 1), (1, 2), (2, 0), (2, 1)))


def place(counts_ref):
    group = lax.axis_index("grp")
    member = lax.axis_index("sub")
    parity = member % 2
    return parity, counts_ref[group, member - parity], counts_ref[group, member]


def pack_kernel(counts_ref, bond_ref, mate_bond_ref, ham_ref, mate_ref, up_ref, down_ref, local_ref, bits_ref):
    parity, low_count, _ = place(counts_ref)
    for t in range(CHIP_COLS):
        in_low = t < low_count
        slot = jnp.where(in_low, t, t - low_count)
        mine = in_low == (parity == 0)
        bonds = jnp.where(mine, bond_ref[pl.ds(slot, 1), :], mate_bond_ref[pl.ds(slot, 1), :]).astype(F32)
        for o in range(5):
            value = jnp.where(mine, ham_ref[slot, o], mate_ref[slot, o])
            if o:
                row = jnp.broadcast_to(bonds[:, o - 1 : o], (1, 128))
                bits_ref[t * 4 + o - 1 : t * 4 + o, :] = row
                value = value * row.astype(BF16)
            local_ref[t * 5 + o] = value
    for k in range(10):
        up_ref[k * 128 : (k + 1) * 128, :] = local_ref[parity * 10 + k]
    up_ref[1280:1296, :] = bits_ref[...].astype(BF16)
    for k in range(5):
        (t, o), (tt, oo) = DOWN[0][k], DOWN[1][k]
        down_ref[k * 128 : (k + 1) * 128, :] = local_ref[jnp.where(parity == 0, t * 5 + o, tt * 5 + oo)]


def main_kernel(
    counts_ref, mu_ref, local_ref, local_bits, up_ref, mate_up_ref, down_ref, mate_down_ref,
    out_hbm, bits, x, first, kept, va, vb, mask, out, out_sems,
):
    parity, _, count = place(counts_ref)
    even = parity == 0

    bits[0:16, :] = up_ref[1280:1296, :].astype(F32)
    bits[16:32, :] = local_bits[...]

    for i in range(3):
        c = 4 + i
        for u in range(12):
            if u == c:
                row = jnp.ones((1, 128), F32)
            elif c < u <= c + 4:
                row = bits[pl.ds((c + parity) * 4 + (u - c - 1), 1), :]
            elif c - 4 <= u < c:
                row = bits[pl.ds((u + parity) * 4 + (c - u - 1), 1), :]
            else:
                row = jnp.zeros((1, 128), F32)
            mask[i : i + 1, u * 128 : (u + 1) * 128] = row

    mu = mu_ref[0]
    eye = (
        lax.broadcasted_iota(jnp.int32, (128, 128), 0) == lax.broadcasted_iota(jnp.int32, (128, 128), 1)
    ).astype(F32)
    zero = jnp.zeros((128, 128), BF16)

    def block(p, o):
        if p < 4:
            rows = slice(((p % 2) * 5 + o) * 128, ((p % 2) * 5 + o + 1) * 128)
            return jnp.where(parity == p // 2, up_ref[rows, :], mate_up_ref[rows, :])
        if p < 8:
            return local_ref[(p - 4) * 5 + o]
        side = 0 if (p - 8, o) in DOWN[0] else 1
        k = DOWN[side].index((p - 8, o))
        rows = slice(k * 128, (k + 1) * 128)
        return jnp.where(parity == side, down_ref[rows, :], mate_down_ref[rows, :])

    def cell(i, j):
        return (slice(i * 128, (i + 1) * 128), slice(j * 128, (j + 1) * 128))

    @pl.when(count > 0)
    def _():
        for p in range(13):
            for q in range(p + 1):
                if p - q > 4 or p == 12:
                    x[cell(p, q)] = zero
                    x[cell(q, p)] = zero
        for p in range(12):
            x[cell(p, p)] = ((block(p, 0).astype(F32) - mu * eye) * 0.25).astype(BF16)
            for o in range(1, 5):
                if p + o < 12:
                    b = block(p, o).astype(F32) * 0.25
                    x[cell(p + o, p)] = b.astype(BF16)
                    x[cell(p, p + o)] = b.T.astype(BF16)

    def at(k):
        return pl.multiple_of(parity * 128 + k, 128)

    span = [(0, 256), (0, 384), (0, 384), (0, 384), (0, 384), (256, 384)]

    def sweep(src, use):
        for n in range(6):
            r0, r1 = span[n]
            k0, k1 = max(0, n - 2), min(6, n + 3)
            acc = jnp.dot(
                src(slice(r0, r1), k0 * 256, k1 * 256),
                x[pl.ds(at(k0 * 256), (k1 - k0) * 256), pl.ds(at(n * 256), 256)],
                preferred_element_type=F32,
            )
            for i in range(r0 // 128, r1 // 128):
                m = mask[i : i + 1, n * 256 : (n + 1) * 256]
                use(i, n, acc[i * 128 - r0 : (i + 1) * 128 - r0, :] * m)

    def of(ref):
        return lambda rows, k0, k1: ref[rows, k0:k1]

    def x_rows(rows, k0, k1):
        return x[pl.ds(at(512 + rows.start), rows.stop - rows.start), pl.ds(at(k0), k1 - k0)]

    for ref in (va, vb):
        ref[256:384, 0:256] = jnp.zeros((128, 256), BF16)
        ref[0:256, 1280:1536] = jnp.zeros((256, 256), BF16)

    def sl(i, n):
        return (slice(i * 128, (i + 1) * 128), slice(n * 256, (n + 1) * 256))

    def store(ref):
        def use(i, n, part):
            ref[sl(i, n)] = part.astype(BF16)

        return use

    pl.when(count > 0)(lambda: sweep(x_rows, store(va)))

    def end_one(i, n, part):
        f = x_rows(slice(i * 128, (i + 1) * 128), n * 256, (n + 1) * 256).astype(F32)
        s = 1.5 * f - 0.5 * part
        kept[sl(i, n)] = s
        vb[sl(i, n)] = s.astype(BF16)

    pl.when(count > 0)(lambda: sweep(of(va), end_one))

    def keep_first(ref):
        def use(i, n, part):
            first[sl(i, n)] = part
            ref[sl(i, n)] = part.astype(BF16)

        return use

    pl.when(count > 0)(lambda: sweep(of(vb), keep_first(va)))
    pl.when(count > 0)(lambda: sweep(of(va), store(vb)))

    def end_two(i, n, part):
        va[sl(i, n)] = (1.5 * first[sl(i, n)] - 0.5 * part).astype(BF16)

    pl.when(count > 0)(lambda: sweep(of(vb), end_two))
    pl.when(count > 0)(lambda: sweep(of(va), keep_first(vb)))
    pl.when(count > 0)(lambda: sweep(of(vb), store(va)))

    turn = jnp.where(jnp.logical_and(parity == 1, count == 1), 1, 0)
    slots = [(i + turn) % 3 for i in range(3)]

    def end_three(i, n, part):
        s3 = 1.5 * first[sl(i, n)] - 0.5 * part
        y = 1.5 * kept[sl(i, n)] - 0.5 * s3
        for h in range(2):
            w = 2 * n + h - i
            if 0 <= w < 9:
                d = -0.5 * y[:, h * 128 : (h + 1) * 128]
                if w == 4:
                    d = d + 0.5 * eye
                d = jnp.where(slots[i] < count, d, 0.0)
                out[slots[i], w] = d.T.astype(BF16)

    pl.when(count > 0)(lambda: sweep(of(va), end_three))
    c = pltpu.make_async_copy(out, out_hbm, out_sems.at[0])
    c.start()
    c.wait()


def shift(value, step):
    size = lax.axis_size("grp") * lax.axis_size("sub")
    return lax.ppermute(value, AXES, [(s, (s + step) % size) for s in range(size)])


def mate_of(value):
    return lax.ppermute(value, "sub", [(s, s ^ 1) for s in range(lax.axis_size("sub"))])


def body(ham_columns, bond_mask, owned_counts, fermi_level):
    smem = pl.BlockSpec(memory_space=pltpu.SMEM)
    vmem = pl.BlockSpec(memory_space=pltpu.VMEM)
    hbm = pl.BlockSpec(memory_space=pltpu.HBM)
    on_chip = lambda *a: [pltpu.with_memory_space_constraint(v, pltpu.VMEM) for v in a]
    mate_bond = mate_of(bond_mask)
    mate_ham = mate_of(ham_columns)
    up, down, local, bits = pl.pallas_call(
        pack_kernel,
        out_shape=(
            pltpu.VMEM((1296, 128), BF16),
            pltpu.VMEM((640, 128), BF16),
            pltpu.VMEM((20, 128, 128), BF16),
            pltpu.VMEM((16, 128), F32),
        ),
        in_specs=[smem, vmem, vmem, vmem, vmem],
        out_specs=(vmem,) * 4,
        name="pack",
    )(owned_counts, bond_mask, *on_chip(mate_bond), ham_columns, *on_chip(mate_ham))
    up_got = shift(up, 2)
    down_got = shift(down, -2)
    up_got, down_got = lax.optimization_barrier((up_got, down_got))
    mate_up = mate_of(up_got)
    mate_down = mate_of(down_got)
    return pl.pallas_call(
        main_kernel,
        out_shape=jax.ShapeDtypeStruct((3, 9, 128, 128), BF16),
        in_specs=[smem, smem] + [vmem] * 6,
        out_specs=hbm,
        scratch_shapes=[
            pltpu.VMEM((32, 128), F32),
            pltpu.VMEM((1664, 1664), BF16),
            pltpu.VMEM((384, 1536), F32),
            pltpu.VMEM((384, 1536), F32),
            pltpu.VMEM((384, 1536), BF16),
            pltpu.VMEM((384, 1536), BF16),
            pltpu.VMEM((8, 1536), F32),
            pltpu.VMEM((3, 9, 128, 128), BF16),
            pltpu.SemaphoreType.DMA((1,)),
        ],
        name="columns",
    )(owned_counts, fermi_level, *on_chip(local, bits, up_got, mate_up, down_got, mate_down))


def solution(mesh):
    placed = (P(AXES, None, None, None), P(AXES, None), P(), P())
    return jax.shard_map(
        body,
        mesh=mesh,
        in_specs=placed,
        out_specs=P(AXES, None, None, None),
        check_vma=False,
    )
```

```python
import jax
import jax.numpy as jnp
from jax import lax
from jax.experimental import pallas as pl
from jax.experimental.pallas import tpu as pltpu
from jax.sharding import PartitionSpec as P


AXES = ("grp", "sub")
CHIP_COLS = 4
BF16 = jnp.bfloat16
F32 = jnp.float32

DOWN = (((0, 0), (0, 1), (1, 0), (0, 2), (0, 3)), ((1, 1), (1, 2), (2, 0), (2, 1), (3, 0)))


def place(counts_ref):
    group = lax.axis_index("grp")
    member = lax.axis_index("sub")
    parity = member % 2
    low = member - parity
    wraps = low == 0
    groups, members = counts_ref.shape
    before_group = jnp.where(wraps, jnp.where(group == 0, groups - 1, group - 1), group)
    before = counts_ref[before_group, jnp.where(wraps, members - 2, low - 2)]
    return parity, counts_ref[group, low], counts_ref[group, member], before


def rest_column(low_count, parity):
    return jnp.where(low_count == 1, 2, 1) + parity


def pack_kernel(counts_ref, bond_ref, mate_bond_ref, ham_ref, mate_ref, up_ref, down_ref, local_ref, bits_ref):
    parity, low_count, _, _ = place(counts_ref)
    for t in range(CHIP_COLS):
        in_low = t < low_count
        slot = jnp.where(in_low, t, t - low_count)
        mine = in_low == (parity == 0)
        bonds = jnp.where(mine, bond_ref[pl.ds(slot, 1), :], mate_bond_ref[pl.ds(slot, 1), :]).astype(F32)
        for o in range(5):
            value = jnp.where(mine, ham_ref[slot, o], mate_ref[slot, o])
            if o:
                row = jnp.broadcast_to(bonds[:, o - 1 : o], (1, 128))
                bits_ref[t * 4 + o - 1 : t * 4 + o, :] = row
                value = value * row.astype(BF16)
            local_ref[t * 5 + o] = value
    rest = rest_column(low_count, parity)
    for k in range(5):
        up_ref[k * 128 : (k + 1) * 128, :] = local_ref[rest * 5 + k]
    up_ref[640:656, :] = bits_ref[...].astype(BF16)
    for k in range(5):
        (t, o), (tt, oo) = DOWN[0][k], DOWN[1][k]
        down_ref[k * 128 : (k + 1) * 128, :] = local_ref[jnp.where(parity == 0, t * 5 + o, tt * 5 + oo)]


def main_kernel(
    counts_ref, mu_ref, local_ref, local_bits, one_ref, mate_one_ref, up_ref, mate_up_ref, down_ref, mate_down_ref,
    keep_ref, send_ref, bits, cols, x, first, kept, va, vb, mask,
):
    parity, _, count, before = place(counts_ref)
    even = parity == 0
    shift = parity * 2

    bits[0:16, :] = up_ref[640:656, :].astype(F32)
    bits[16:32, :] = local_bits[...]

    def lane(own, mate, which):
        return jnp.where(parity == which, own, mate)

    for which in range(2):
        p = jnp.where(before == 1, 1, 3) if which else 0
        for o in range(5):
            value = lane(one_ref[0, o], mate_one_ref[0, o], which)
            if o:
                value = value * bits[pl.ds(p * 4 + o - 1, 1), :].astype(BF16)
            cols[p, o] = value
        p = rest_column(before, which)
        for o in range(5):
            rows = slice(o * 128, (o + 1) * 128)
            cols[p, o] = lane(up_ref[rows, :], mate_up_ref[rows, :], which)
        for k, (t, o) in enumerate(DOWN[which]):
            rows = slice(k * 128, (k + 1) * 128)
            cols[8 + t, o] = lane(down_ref[rows, :], mate_down_ref[rows, :], which)
    for t in range(CHIP_COLS):
        for o in range(5):
            cols[4 + t, o] = local_ref[t * 5 + o]

    for i in range(2):
        c = 4 + i
        for u in range(10):
            if u == c:
                row = jnp.ones((1, 128), F32)
            elif c < u <= c + 4:
                row = bits[pl.ds((c + shift) * 4 + (u - c - 1), 1), :]
            elif c - 4 <= u < c:
                row = bits[pl.ds((u + shift) * 4 + (c - u - 1), 1), :]
            else:
                row = jnp.zeros((1, 128), F32)
            mask[i : i + 1, u * 128 : (u + 1) * 128] = row

    mu = mu_ref[0]
    eye = (
        lax.broadcasted_iota(jnp.int32, (128, 128), 0) == lax.broadcasted_iota(jnp.int32, (128, 128), 1)
    ).astype(F32)
    zero = jnp.zeros((128, 128), BF16)

    def cell(i, j):
        return (slice(i * 128, (i + 1) * 128), slice(j * 128, (j + 1) * 128))

    @pl.when(count > 0)
    def _():
        for u in range(10):
            for v in range(u - 4):
                x[cell(u, v)] = zero
                x[cell(v, u)] = zero
        for u in range(10):
            x[cell(u, u)] = ((cols[u + shift, 0].astype(F32) - mu * eye) * 0.25).astype(BF16)
            for o in range(1, 5):
                if u + o < 10:
                    b = cols[u + shift, o] * jnp.asarray(0.25, BF16)
                    x[cell(u + o, u)] = b
                    x[cell(u, u + o)] = b.T

    def sweep(src, off, use):
        for n in range(5):
            k0, k1 = max(0, n - 2), min(5, n + 3)
            acc = jnp.dot(
                src[off : off + 256, k0 * 256 : k1 * 256],
                x[k0 * 256 : k1 * 256, n * 256 : (n + 1) * 256],
                preferred_element_type=F32,
            )
            for i in range(2):
                m = mask[i : i + 1, n * 256 : (n + 1) * 256]
                use(i, n, acc[i * 128 : (i + 1) * 128, :] * m)

    def sl(i, n):
        return (slice(i * 128, (i + 1) * 128), slice(n * 256, (n + 1) * 256))

    def store(ref):
        def use(i, n, part):
            ref[sl(i, n)] = part.astype(BF16)

        return use

    def end_one(i, n, part):
        f = x[512 + i * 128 : 512 + (i + 1) * 128, n * 256 : (n + 1) * 256].astype(F32)
        s = 1.5 * f - 0.5 * part
        kept[sl(i, n)] = s
        vb[sl(i, n)] = s.astype(BF16)

    def keep_first(ref):
        def use(i, n, part):
            first[sl(i, n)] = part
            ref[sl(i, n)] = part.astype(BF16)

        return use

    def end_two(i, n, part):
        va[sl(i, n)] = (1.5 * first[sl(i, n)] - 0.5 * part).astype(BF16)

    def end_three(targets):
        def use(i, n, part):
            s3 = 1.5 * first[sl(i, n)] - 0.5 * part
            y = 1.5 * kept[sl(i, n)] - 0.5 * s3
            for h in range(2):
                w = 2 * n + h - i
                if 0 <= w < 9:
                    d = -0.5 * y[:, h * 128 : (h + 1) * 128]
                    if w == 4:
                        d = d + 0.5 * eye
                    targets[i][w] = d.astype(BF16).T

        return use

    pl.when(count > 0)(lambda: sweep(x, 512, store(va)))
    pl.when(count > 0)(lambda: sweep(va, 0, end_one))
    pl.when(count > 0)(lambda: sweep(vb, 0, keep_first(va)))
    pl.when(count > 0)(lambda: sweep(va, 0, store(vb)))
    pl.when(count > 0)(lambda: sweep(vb, 0, end_two))
    pl.when(count > 0)(lambda: sweep(va, 0, keep_first(vb)))
    pl.when(count > 0)(lambda: sweep(vb, 0, store(va)))
    pl.when(even)(lambda: sweep(va, 0, end_three((keep_ref, send_ref))))
    pl.when(jnp.logical_not(even))(lambda: sweep(va, 0, end_three((send_ref, keep_ref))))


def place_kernel(counts_ref, keep_ref, send_ref, got_ref, out_hbm, zeros, sems):
    parity, _, count, _ = place(counts_ref)
    three = count == 3
    own = pltpu.make_async_copy(keep_ref, out_hbm.at[jnp.where(three, parity * 2, 0)], sems.at[0])
    own.start()

    @pl.when(three)
    def _():
        a = pltpu.make_async_copy(send_ref, out_hbm.at[1], sems.at[1])
        b = pltpu.make_async_copy(got_ref, out_hbm.at[2 - parity * 2], sems.at[2])
        a.start()
        b.start()
        a.wait()
        b.wait()

    @pl.when(jnp.logical_not(three))
    def _():
        zeros[...] = jnp.zeros(zeros.shape, BF16)
        a = pltpu.make_async_copy(zeros, out_hbm.at[1], sems.at[1])
        b = pltpu.make_async_copy(zeros, out_hbm.at[2], sems.at[2])
        a.start()
        b.start()
        a.wait()
        b.wait()

    own.wait()


def shift(value, step):
    size = lax.axis_size("grp") * lax.axis_size("sub")
    return lax.ppermute(value, AXES, [(s, (s + step) % size) for s in range(size)])


def mate_of(value):
    return lax.ppermute(value, "sub", [(s, s ^ 1) for s in range(lax.axis_size("sub"))])


def body(ham_columns, bond_mask, owned_counts, fermi_level):
    smem = pl.BlockSpec(memory_space=pltpu.SMEM)
    vmem = pl.BlockSpec(memory_space=pltpu.VMEM)
    hbm = pl.BlockSpec(memory_space=pltpu.HBM)
    on_chip = lambda *a: [pltpu.with_memory_space_constraint(v, pltpu.VMEM) for v in a]
    mate_bond = mate_of(bond_mask)
    mate_ham = mate_of(ham_columns)
    one_got = shift(ham_columns[0:1], 2)
    up, down, local, bits = pl.pallas_call(
        pack_kernel,
        out_shape=(
            pltpu.VMEM((656, 128), BF16),
            pltpu.VMEM((640, 128), BF16),
            pltpu.VMEM((20, 128, 128), BF16),
            pltpu.VMEM((16, 128), F32),
        ),
        in_specs=[smem, vmem, vmem, vmem, vmem],
        out_specs=(vmem,) * 4,
        name="pack",
    )(owned_counts, bond_mask, *on_chip(mate_bond), ham_columns, *on_chip(mate_ham))
    up_got = shift(up, 2)
    down_got = shift(down, -2)
    up_got, down_got = lax.optimization_barrier((up_got, down_got))
    mate_one = mate_of(one_got)
    mate_up = mate_of(up_got)
    mate_down = mate_of(down_got)
    keep, send = pl.pallas_call(
        main_kernel,
        out_shape=(pltpu.VMEM((9, 128, 128), BF16),) * 2,
        in_specs=[smem, smem] + [vmem] * 8,
        out_specs=(vmem,) * 2,
        scratch_shapes=[
            pltpu.VMEM((32, 128), F32),
            pltpu.VMEM((12, 5, 128, 128), BF16),
            pltpu.VMEM((1280, 1280), BF16),
            pltpu.VMEM((256, 1280), F32),
            pltpu.VMEM((256, 1280), F32),
            pltpu.VMEM((256, 1280), BF16),
            pltpu.VMEM((256, 1280), BF16),
            pltpu.VMEM((8, 1280), F32),
        ],
        name="columns",
    )(
        owned_counts,
        fermi_level,
        *on_chip(local, bits, one_got, mate_one, up_got, mate_up, down_got, mate_down),
    )
    got = mate_of(send)
    return pl.pallas_call(
        place_kernel,
        out_shape=jax.ShapeDtypeStruct((3, 9, 128, 128), BF16),
        in_specs=[smem] + [vmem] * 3,
        out_specs=hbm,
        scratch_shapes=[pltpu.VMEM((9, 128, 128), BF16), pltpu.SemaphoreType.DMA((3,))],
        name="place",
    )(owned_counts, *on_chip(keep, send, got))


def solution(mesh):
    placed = (P(AXES, None, None, None), P(AXES, None), P(), P())
    return jax.shard_map(
        body,
        mesh=mesh,
        in_specs=placed,
        out_specs=P(AXES, None, None, None),
        check_vma=False,
    )
```

```python
import jax
import jax.numpy as jnp
from jax import lax
from jax.experimental import pallas as pl
from jax.experimental.pallas import tpu as pltpu
from jax.sharding import PartitionSpec as P


AXES = ("grp", "sub")
CHIP_COLS = 4
BF16 = jnp.bfloat16
F32 = jnp.float32

DOWN = (((0, 0), (0, 1), (1, 0), (0, 2), (0, 3)), ((1, 1), (1, 2), (2, 0), (2, 1), (3, 0)))


def place(counts_ref):
    group = lax.axis_index("grp")
    member = lax.axis_index("sub")
    parity = member % 2
    low = member - parity
    wraps = low == 0
    groups, members = counts_ref.shape
    before_group = jnp.where(wraps, jnp.where(group == 0, groups - 1, group - 1), group)
    before = counts_ref[before_group, jnp.where(wraps, members - 2, low - 2)]
    return parity, counts_ref[group, low], counts_ref[group, member], before


def rest_column(low_count, parity):
    return jnp.where(low_count == 1, 2, 1) + parity


def pack_kernel(counts_ref, bond_ref, mate_bond_ref, ham_ref, mate_ref, up_ref, down_ref, local_ref, bits_ref):
    parity, low_count, _, _ = place(counts_ref)
    for t in range(CHIP_COLS):
        in_low = t < low_count
        slot = jnp.where(in_low, t, t - low_count)
        mine = in_low == (parity == 0)
        bonds = jnp.where(mine, bond_ref[pl.ds(slot, 1), :], mate_bond_ref[pl.ds(slot, 1), :]).astype(F32)
        for o in range(5):
            value = jnp.where(mine, ham_ref[slot, o], mate_ref[slot, o])
            if o:
                row = jnp.broadcast_to(bonds[:, o - 1 : o], (1, 128))
                bits_ref[t * 4 + o - 1 : t * 4 + o, :] = row
                value = value * row.astype(BF16)
            local_ref[t * 5 + o] = value
    rest = rest_column(low_count, parity)
    for k in range(5):
        up_ref[k * 128 : (k + 1) * 128, :] = local_ref[rest * 5 + k]
    up_ref[640:656, :] = bits_ref[...].astype(BF16)
    for k in range(5):
        (t, o), (tt, oo) = DOWN[0][k], DOWN[1][k]
        down_ref[k * 128 : (k + 1) * 128, :] = local_ref[jnp.where(parity == 0, t * 5 + o, tt * 5 + oo)]


def main_kernel(
    counts_ref, mu_ref, local_ref, local_bits, one_ref, mate_one_ref, up_ref, mate_up_ref, down_ref, mate_down_ref,
    keep_ref, send_ref, bits, cols, x, first, kept, va, vb, mask,
):
    parity, _, count, before = place(counts_ref)
    even = parity == 0
    shift = parity * 2

    bits[0:16, :] = up_ref[640:656, :].astype(F32)
    bits[16:32, :] = local_bits[...]

    def lane(own, mate, which):
        return jnp.where(parity == which, own, mate)

    for which in range(2):
        p = jnp.where(before == 1, 1, 3) if which else 0
        for o in range(5):
            value = lane(one_ref[0, o], mate_one_ref[0, o], which)
            if o:
                value = value * bits[pl.ds(p * 4 + o - 1, 1), :].astype(BF16)
            cols[p, o] = value
        p = rest_column(before, which)
        for o in range(5):
            rows = slice(o * 128, (o + 1) * 128)
            cols[p, o] = lane(up_ref[rows, :], mate_up_ref[rows, :], which)
        for k, (t, o) in enumerate(DOWN[which]):
            rows = slice(k * 128, (k + 1) * 128)
            cols[8 + t, o] = lane(down_ref[rows, :], mate_down_ref[rows, :], which)
    for t in range(CHIP_COLS):
        for o in range(5):
            cols[4 + t, o] = local_ref[t * 5 + o]

    for i in range(2):
        c = 4 + i
        for u in range(10):
            if u == c:
                row = jnp.ones((1, 128), F32)
            elif c < u <= c + 4:
                row = bits[pl.ds((c + shift) * 4 + (u - c - 1), 1), :]
            elif c - 4 <= u < c:
                row = bits[pl.ds((u + shift) * 4 + (c - u - 1), 1), :]
            else:
                row = jnp.zeros((1, 128), F32)
            mask[i : i + 1, u * 128 : (u + 1) * 128] = row

    mu = mu_ref[0]
    eye = (
        lax.broadcasted_iota(jnp.int32, (128, 128), 0) == lax.broadcasted_iota(jnp.int32, (128, 128), 1)
    ).astype(F32)
    zero = jnp.zeros((128, 128), BF16)

    def cell(i, j):
        return (slice(i * 128, (i + 1) * 128), slice(j * 128, (j + 1) * 128))

    @pl.when(count > 0)
    def _():
        for u in range(10):
            for v in range(u - 4):
                x[cell(u, v)] = zero
                x[cell(v, u)] = zero
        for u in range(10):
            x[cell(u, u)] = ((cols[u + shift, 0].astype(F32) - mu * eye) * 0.25).astype(BF16)
            for o in range(1, 5):
                if u + o < 10:
                    b = cols[u + shift, o] * jnp.asarray(0.25, BF16)
                    x[cell(u + o, u)] = b
                    x[cell(u, u + o)] = b.T

    def sweep(src, off, use):
        for n in range(5):
            k0, k1 = max(0, n - 2), min(5, n + 3)
            acc = jnp.dot(
                src[off : off + 256, k0 * 256 : k1 * 256],
                x[k0 * 256 : k1 * 256, n * 256 : (n + 1) * 256],
                preferred_element_type=F32,
            )
            for i in range(2):
                m = mask[i : i + 1, n * 256 : (n + 1) * 256]
                use(i, n, acc[i * 128 : (i + 1) * 128, :] * m)

    def sl(i, n):
        return (slice(i * 128, (i + 1) * 128), slice(n * 256, (n + 1) * 256))

    def store(ref):
        def use(i, n, part):
            ref[sl(i, n)] = part.astype(BF16)

        return use

    def end_one(i, n, part):
        f = x[512 + i * 128 : 512 + (i + 1) * 128, n * 256 : (n + 1) * 256].astype(F32)
        s = 1.5 * f - 0.5 * part
        kept[sl(i, n)] = s
        vb[sl(i, n)] = s.astype(BF16)

    def keep_first(ref):
        def use(i, n, part):
            first[sl(i, n)] = part
            ref[sl(i, n)] = part.astype(BF16)

        return use

    def end_two(i, n, part):
        va[sl(i, n)] = (1.5 * first[sl(i, n)] - 0.5 * part).astype(BF16)

    def end_three(targets):
        def use(i, n, part):
            s3 = 1.5 * first[sl(i, n)] - 0.5 * part
            y = 1.5 * kept[sl(i, n)] - 0.5 * s3
            for h in range(2):
                w = 2 * n + h - i
                if 0 <= w < 9:
                    d = -0.5 * y[:, h * 128 : (h + 1) * 128]
                    if w == 4:
                        d = d + 0.5 * eye
                    targets[i][w] = d.astype(BF16).T

        return use

    @pl.when(count > 0)
    def _():
        sweep(x, 512, store(va))
        sweep(va, 0, end_one)
        sweep(vb, 0, keep_first(va))
        sweep(va, 0, store(vb))
        sweep(vb, 0, end_two)
        sweep(va, 0, keep_first(vb))
        sweep(vb, 0, store(va))

    pl.when(even)(lambda: sweep(va, 0, end_three((keep_ref, send_ref))))
    pl.when(jnp.logical_not(even))(lambda: sweep(va, 0, end_three((send_ref, keep_ref))))


def put_kernel(counts_ref, keep_ref, send_ref, out_hbm, zeros, sems):
    parity, _, count, _ = place(counts_ref)
    three = count == 3
    own = pltpu.make_async_copy(keep_ref, out_hbm.at[jnp.where(three, parity * 2, 0)], sems.at[0])
    own.start()

    @pl.when(three)
    def _():
        a = pltpu.make_async_copy(send_ref, out_hbm.at[1], sems.at[1])
        a.start()
        a.wait()

    @pl.when(jnp.logical_not(three))
    def _():
        zeros[...] = jnp.zeros(zeros.shape, BF16)
        a = pltpu.make_async_copy(zeros, out_hbm.at[1], sems.at[1])
        a.start()
        a.wait()

    own.wait()


def shift(value, step):
    size = lax.axis_size("grp") * lax.axis_size("sub")
    return lax.ppermute(value, AXES, [(s, (s + step) % size) for s in range(size)])


def mate_of(value):
    return lax.ppermute(value, "sub", [(s, s ^ 1) for s in range(lax.axis_size("sub"))])


def body(ham_columns, bond_mask, owned_counts, fermi_level):
    smem = pl.BlockSpec(memory_space=pltpu.SMEM)
    vmem = pl.BlockSpec(memory_space=pltpu.VMEM)
    hbm = pl.BlockSpec(memory_space=pltpu.HBM)
    on_chip = lambda *a: [pltpu.with_memory_space_constraint(v, pltpu.VMEM) for v in a]
    mate_bond = mate_of(bond_mask)
    mate_ham = mate_of(ham_columns)
    one_got = shift(ham_columns[0:1], 2)
    up, down, local, bits = pl.pallas_call(
        pack_kernel,
        out_shape=(
            pltpu.VMEM((656, 128), BF16),
            pltpu.VMEM((640, 128), BF16),
            pltpu.VMEM((20, 128, 128), BF16),
            pltpu.VMEM((16, 128), F32),
        ),
        in_specs=[smem, vmem, vmem, vmem, vmem],
        out_specs=(vmem,) * 4,
        name="pack",
    )(owned_counts, bond_mask, *on_chip(mate_bond), ham_columns, *on_chip(mate_ham))
    up_got = shift(up, 2)
    down_got = shift(down, -2)
    mate_one = mate_of(one_got)
    mate_down = mate_of(down_got)
    parity, _, count, _ = place(owned_counts)
    three = count == 3
    slot = jnp.where(jnp.logical_and(three, parity == 1), 0, 2)
    up_got, mate_one, mate_down, three, slot = lax.optimization_barrier((up_got, mate_one, mate_down, three, slot))
    mate_up = mate_of(up_got)
    keep, send = pl.pallas_call(
        main_kernel,
        out_shape=(pltpu.VMEM((9, 128, 128), BF16),) * 2,
        in_specs=[smem, smem] + [vmem] * 8,
        out_specs=(vmem,) * 2,
        scratch_shapes=[
            pltpu.VMEM((32, 128), F32),
            pltpu.VMEM((12, 5, 128, 128), BF16),
            pltpu.VMEM((1280, 1280), BF16),
            pltpu.VMEM((256, 1280), F32),
            pltpu.VMEM((256, 1280), F32),
            pltpu.VMEM((256, 1280), BF16),
            pltpu.VMEM((256, 1280), BF16),
            pltpu.VMEM((8, 1280), F32),
        ],
        name="columns",
    )(
        owned_counts,
        fermi_level,
        *on_chip(local, bits, one_got, mate_one, up_got, mate_up, down_got, mate_down),
    )
    got = mate_of(send)
    shape = jax.ShapeDtypeStruct((3, 9, 128, 128), BF16)
    partial = pl.pallas_call(
        put_kernel,
        out_shape=shape,
        in_specs=[smem, vmem, vmem],
        out_specs=hbm,
        scratch_shapes=[pltpu.VMEM((9, 128, 128), BF16), pltpu.SemaphoreType.DMA((3,))],
        name="put",
    )(owned_counts, *on_chip(keep, send))
    last = jnp.where(three, got, jnp.zeros_like(got))
    return lax.dynamic_update_slice(partial, last[None], (slot, 0, 0, 0))


def solution(mesh):
    placed = (P(AXES, None, None, None), P(AXES, None), P(), P())
    return jax.shard_map(
        body,
        mesh=mesh,
        in_specs=placed,
        out_specs=P(AXES, None, None, None),
        check_vma=False,
    )
```

```python
import jax
import jax.numpy as jnp
from jax import lax
from jax.experimental import pallas as pl
from jax.experimental.pallas import tpu as pltpu
from jax.sharding import PartitionSpec as P


AXES = ("grp", "sub")
CHIP_COLS = 4
BF16 = jnp.bfloat16
F32 = jnp.float32

DOWN = (((0, 0), (0, 1), (1, 0), (0, 2), (0, 3)), ((1, 1), (1, 2), (2, 0), (2, 1), (3, 0)))


def place(counts_ref):
    group = lax.axis_index("grp")
    member = lax.axis_index("sub")
    parity = member % 2
    low = member - parity
    wraps = low == 0
    groups, members = counts_ref.shape
    before_group = jnp.where(wraps, jnp.where(group == 0, groups - 1, group - 1), group)
    before = counts_ref[before_group, jnp.where(wraps, members - 2, low - 2)]
    return parity, counts_ref[group, low], counts_ref[group, member], before


def rest_column(low_count, parity):
    return jnp.where(low_count == 1, 2, 1) + parity


def pack_kernel(counts_ref, bond_ref, mate_bond_ref, ham_ref, mate_ref, up_ref, down_ref, local_ref, bits_ref, slot_ref, three_ref):
    parity, low_count, count, _ = place(counts_ref)
    three_ref[0] = jnp.where(count == 3, 1, 0)
    slot_ref[0] = jnp.where(jnp.logical_and(count == 3, parity == 1), 0, 2)
    for t in range(CHIP_COLS):
        in_low = t < low_count
        slot = jnp.where(in_low, t, t - low_count)
        mine = in_low == (parity == 0)
        bonds = jnp.where(mine, bond_ref[pl.ds(slot, 1), :], mate_bond_ref[pl.ds(slot, 1), :]).astype(F32)
        for o in range(5):
            value = jnp.where(mine, ham_ref[slot, o], mate_ref[slot, o])
            if o:
                row = jnp.broadcast_to(bonds[:, o - 1 : o], (1, 128))
                bits_ref[t * 4 + o - 1 : t * 4 + o, :] = row
                value = value * row.astype(BF16)
            local_ref[t * 5 + o] = value
    rest = rest_column(low_count, parity)
    for k in range(5):
        up_ref[k * 128 : (k + 1) * 128, :] = local_ref[rest * 5 + k]
    up_ref[640:656, :] = bits_ref[...].astype(BF16)
    for k in range(5):
        (t, o), (tt, oo) = DOWN[0][k], DOWN[1][k]
        down_ref[k * 128 : (k + 1) * 128, :] = local_ref[jnp.where(parity == 0, t * 5 + o, tt * 5 + oo)]


def main_kernel(
    counts_ref, mu_ref, local_ref, local_bits, one_ref, mate_one_ref, up_ref, mate_up_ref, down_ref, mate_down_ref,
    keep_ref, send_ref, bits, cols, x, first, kept, va, vb, mask,
):
    parity, _, count, before = place(counts_ref)
    even = parity == 0
    shift = parity * 2

    bits[0:16, :] = up_ref[640:656, :].astype(F32)
    bits[16:32, :] = local_bits[...]

    def lane(own, mate, which):
        return jnp.where(parity == which, own, mate)

    for which in range(2):
        p = jnp.where(before == 1, 1, 3) if which else 0
        for o in range(5):
            value = lane(one_ref[0, o], mate_one_ref[0, o], which)
            if o:
                value = value * bits[pl.ds(p * 4 + o - 1, 1), :].astype(BF16)
            cols[p, o] = value
        p = rest_column(before, which)
        for o in range(5):
            rows = slice(o * 128, (o + 1) * 128)
            cols[p, o] = lane(up_ref[rows, :], mate_up_ref[rows, :], which)
        for k, (t, o) in enumerate(DOWN[which]):
            rows = slice(k * 128, (k + 1) * 128)
            cols[8 + t, o] = lane(down_ref[rows, :], mate_down_ref[rows, :], which)
    for t in range(CHIP_COLS):
        for o in range(5):
            cols[4 + t, o] = local_ref[t * 5 + o]

    for i in range(2):
        c = 4 + i
        for u in range(10):
            if u == c:
                row = jnp.ones((1, 128), F32)
            elif c < u <= c + 4:
                row = bits[pl.ds((c + shift) * 4 + (u - c - 1), 1), :]
            elif c - 4 <= u < c:
                row = bits[pl.ds((u + shift) * 4 + (c - u - 1), 1), :]
            else:
                row = jnp.zeros((1, 128), F32)
            mask[i : i + 1, u * 128 : (u + 1) * 128] = row

    mu = mu_ref[0]
    eye = (
        lax.broadcasted_iota(jnp.int32, (128, 128), 0) == lax.broadcasted_iota(jnp.int32, (128, 128), 1)
    ).astype(F32)
    zero = jnp.zeros((128, 128), BF16)

    def cell(i, j):
        return (slice(i * 128, (i + 1) * 128), slice(j * 128, (j + 1) * 128))

    @pl.when(count > 0)
    def _():
        for u in range(10):
            for v in range(u - 4):
                x[cell(u, v)] = zero
                x[cell(v, u)] = zero
        for u in range(10):
            x[cell(u, u)] = ((cols[u + shift, 0].astype(F32) - mu * eye) * 0.25).astype(BF16)
            for o in range(1, 5):
                if u + o < 10:
                    b = cols[u + shift, o] * jnp.asarray(0.25, BF16)
                    x[cell(u + o, u)] = b
                    x[cell(u, u + o)] = b.T

    def sweep(src, off, use):
        for n in range(5):
            k0, k1 = max(0, n - 2), min(5, n + 3)
            acc = jnp.dot(
                src[off : off + 256, k0 * 256 : k1 * 256],
                x[k0 * 256 : k1 * 256, n * 256 : (n + 1) * 256],
                preferred_element_type=F32,
            )
            for i in range(2):
                m = mask[i : i + 1, n * 256 : (n + 1) * 256]
                use(i, n, acc[i * 128 : (i + 1) * 128, :] * m)

    def sl(i, n):
        return (slice(i * 128, (i + 1) * 128), slice(n * 256, (n + 1) * 256))

    def store(ref):
        def use(i, n, part):
            ref[sl(i, n)] = part.astype(BF16)

        return use

    def end_one(i, n, part):
        f = x[512 + i * 128 : 512 + (i + 1) * 128, n * 256 : (n + 1) * 256].astype(F32)
        s = 1.5 * f - 0.5 * part
        kept[sl(i, n)] = s
        vb[sl(i, n)] = s.astype(BF16)

    def keep_first(ref):
        def use(i, n, part):
            first[sl(i, n)] = part
            ref[sl(i, n)] = part.astype(BF16)

        return use

    def end_two(i, n, part):
        va[sl(i, n)] = (1.5 * first[sl(i, n)] - 0.5 * part).astype(BF16)

    def end_three(targets):
        def use(i, n, part):
            s3 = 1.5 * first[sl(i, n)] - 0.5 * part
            y = 1.5 * kept[sl(i, n)] - 0.5 * s3
            for h in range(2):
                w = 2 * n + h - i
                if 0 <= w < 9:
                    d = -0.5 * y[:, h * 128 : (h + 1) * 128]
                    if w == 4:
                        d = d + 0.5 * eye
                    targets[i][w] = d.astype(BF16).T

        return use

    @pl.when(count > 0)
    def _():
        sweep(x, 512, store(va))
        sweep(va, 0, end_one)
        sweep(vb, 0, keep_first(va))
        sweep(va, 0, store(vb))
        sweep(vb, 0, end_two)
        sweep(va, 0, keep_first(vb))
        sweep(vb, 0, store(va))

    pl.when(even)(lambda: sweep(va, 0, end_three((keep_ref, send_ref))))
    pl.when(jnp.logical_not(even))(lambda: sweep(va, 0, end_three((send_ref, keep_ref))))


def put_kernel(counts_ref, keep_ref, send_ref, out_hbm, zeros, sems):
    parity, _, count, _ = place(counts_ref)
    three = count == 3
    own = pltpu.make_async_copy(keep_ref, out_hbm.at[jnp.where(three, parity * 2, 0)], sems.at[0])
    own.start()

    @pl.when(three)
    def _():
        a = pltpu.make_async_copy(send_ref, out_hbm.at[1], sems.at[1])
        a.start()
        a.wait()

    @pl.when(jnp.logical_not(three))
    def _():
        zeros[...] = jnp.zeros(zeros.shape, BF16)
        a = pltpu.make_async_copy(zeros, out_hbm.at[1], sems.at[1])
        a.start()
        a.wait()

    own.wait()


def shift(value, step):
    size = lax.axis_size("grp") * lax.axis_size("sub")
    return lax.ppermute(value, AXES, [(s, (s + step) % size) for s in range(size)])


def mate_of(value):
    return lax.ppermute(value, "sub", [(s, s ^ 1) for s in range(lax.axis_size("sub"))])


def body(ham_columns, bond_mask, owned_counts, fermi_level):
    smem = pl.BlockSpec(memory_space=pltpu.SMEM)
    vmem = pl.BlockSpec(memory_space=pltpu.VMEM)
    hbm = pl.BlockSpec(memory_space=pltpu.HBM)
    on_chip = lambda *a: [pltpu.with_memory_space_constraint(v, pltpu.VMEM) for v in a]
    mate_bond = mate_of(bond_mask)
    mate_ham = mate_of(ham_columns)
    one_got = shift(ham_columns[0:1], 2)
    up, down, local, bits, slot, three = pl.pallas_call(
        pack_kernel,
        out_shape=(
            pltpu.VMEM((656, 128), BF16),
            pltpu.VMEM((640, 128), BF16),
            pltpu.VMEM((20, 128, 128), BF16),
            pltpu.VMEM((16, 128), F32),
            jax.ShapeDtypeStruct((1,), jnp.int32),
            jax.ShapeDtypeStruct((1,), jnp.int32),
        ),
        in_specs=[smem, vmem, vmem, vmem, vmem],
        out_specs=(vmem,) * 4 + (smem,) * 2,
        name="pack",
    )(owned_counts, bond_mask, *on_chip(mate_bond), ham_columns, *on_chip(mate_ham))
    up_got = shift(up, 2)
    down_got = shift(down, -2)
    mate_one = mate_of(one_got)
    mate_down = mate_of(down_got)
    up_got, mate_one, mate_down = lax.optimization_barrier((up_got, mate_one, mate_down))
    mate_up = mate_of(up_got)
    keep, send = pl.pallas_call(
        main_kernel,
        out_shape=(pltpu.VMEM((9, 128, 128), BF16),) * 2,
        in_specs=[smem, smem] + [vmem] * 8,
        out_specs=(vmem,) * 2,
        scratch_shapes=[
            pltpu.VMEM((32, 128), F32),
            pltpu.VMEM((12, 5, 128, 128), BF16),
            pltpu.VMEM((1280, 1280), BF16),
            pltpu.VMEM((256, 1280), F32),
            pltpu.VMEM((256, 1280), F32),
            pltpu.VMEM((256, 1280), BF16),
            pltpu.VMEM((256, 1280), BF16),
            pltpu.VMEM((8, 1280), F32),
        ],
        name="columns",
    )(
        owned_counts,
        fermi_level,
        *on_chip(local, bits, one_got, mate_one, up_got, mate_up, down_got, mate_down),
    )
    got = mate_of(send)
    shape = jax.ShapeDtypeStruct((3, 9, 128, 128), BF16)
    partial = pl.pallas_call(
        put_kernel,
        out_shape=shape,
        in_specs=[smem, vmem, vmem],
        out_specs=hbm,
        scratch_shapes=[pltpu.VMEM((9, 128, 128), BF16), pltpu.SemaphoreType.DMA((3,))],
        name="put",
    )(owned_counts, *on_chip(keep, send))
    last = jnp.where(three[0] == 1, got, jnp.zeros_like(got))
    return lax.dynamic_update_slice(partial, last[None], (slot[0], 0, 0, 0))


def solution(mesh):
    placed = (P(AXES, None, None, None), P(AXES, None), P(), P())
    return jax.shard_map(
        body,
        mesh=mesh,
        in_specs=placed,
        out_specs=P(AXES, None, None, None),
        check_vma=False,
    )
```
